128 devices in a mesh: lat: 4 (over z), lon: 32 (over x, y, core).
Axes of the slice: x: 4, y: 4, z: 4, core: 2. Of those that a mesh axis runs over, the one named last changes fastest.
Arguments:
- fields: bfloat16 [3, 2048, 32, 384], P(None, ('lat', 'lon')), may hold values from -6 to 6
- weights: bfloat16 [3, 4096, 8, 32, 128], P(None, ('lat', 'lon')), may hold values from -0.5 to 0.5
- pair_slots: int32 [3, 4096, 8], P(None, ('lat', 'lon')), may hold values from 0 to 15
- pair_counts: int32 [3, 4096], P(None, ('lat', 'lon')), may hold values from 1 to 8
- requests: int32 [3, 128, 16], replicated, may hold values from 0 to 2047, as said below
- eofs: bfloat16 [200, 524288], P(None, ('lat', 'lon')), may hold values from -0.0078125 to 0.0078125
Outputs:
- pcs: float32 [200, 1152], P(None, ('lat', 'lon'))
The draws below stay inside these ranges and needn't reach their ends.
Inputs may be any that keep to these rules, and one draw needn't show every extreme that they name: requests[g, d] lists 16 distinct source tiles for grid g and device d (d = lat index * lon devices + lon index); source tile j lies on device j // 16; all of them lie on devices with d's lat index whose lon index is d's own or one of its two cyclic neighbours, at most 8 on any one device, and exactly 8 on some device for every g and d. `pair_slots`: only entries with p < pair_counts[g, t] are used.
All inputs are finite; a program needn't handle non-finite values.
Results may differ from the reference program's by a relative error of at most 0.0029.
Values may be sent and summed in bfloat16 or wider, within the bound.
A program may use at most 128 MiB of HBM per device.

```python
import jax
import jax.numpy as jnp
from jax import lax

EOFS = 200
TT = 128
TS = 32
MAXP = 8
MONTHS = 24
GRIDS = 3
MODELS_G = 16
TILES_DEV = 32
STILES_DEV = 16
REQ = 16
CAP = 8
GCOLS = 384
TARGET_TILES = 4096
CELLS = 524288
SRC_TILES = 2048
N_LAT = 4
N_LON = 32


def draw_requests(key, part):
    device_total = N_LAT * N_LON
    keys_all = jax.random.split(key, 4)
    heavy = jax.random.randint(keys_all[0], (GRIDS, device_total), 0, 3)
    offsets = jax.random.randint(keys_all[1], (GRIDS, device_total, 3), 0, STILES_DEV)
    perm_keys = jax.random.split(keys_all[2], GRIDS * device_total)
    others = jax.vmap(lambda single: jax.random.permutation(single, 2 * CAP)[:REQ - CAP])(perm_keys)
    others = others.reshape(GRIDS, device_total, REQ - CAP)
    order_keys = jax.random.split(keys_all[3], GRIDS * device_total)
    orders = jax.vmap(lambda single: jax.random.permutation(single, REQ))(order_keys).reshape(GRIDS, device_total, REQ)
    first_rel = jnp.broadcast_to(heavy[:, :, None], (GRIDS, device_total, CAP))
    first_rank = jnp.broadcast_to(jnp.arange(CAP, dtype=jnp.int32)[None, None, :], (GRIDS, device_total, CAP))
    other_index = others // CAP
    other_rel = other_index + (other_index >= heavy[:, :, None]).astype(jnp.int32)
    other_rank = others % CAP
    relative = jnp.concatenate([first_rel, other_rel], axis=2).astype(jnp.int32)
    ranking = jnp.concatenate([first_rank, other_rank], axis=2).astype(jnp.int32)
    chosen_offset = jnp.take_along_axis(offsets, relative, axis=2)
    local_tile = (chosen_offset + ranking) % STILES_DEV
    devices = jnp.arange(device_total, dtype=jnp.int32)[None, :, None]
    band = devices // N_LON
    sector = (devices % N_LON + relative - 1 + N_LON) % N_LON
    tiles = (band * N_LON + sector) * STILES_DEV + local_tile
    tiles = jnp.take_along_axis(tiles, orders, axis=2)
    return tiles.astype(jnp.int32)


def with_ends(drawn, key, smallest, top_value):
    longest = drawn.shape.index(max(drawn.shape))
    spots = []
    for shift in (0, 1):
        where = [jax.random.randint(jax.random.fold_in(key, axis), (), 0, length) for axis, length in enumerate(drawn.shape)]
        where[longest] = (where[longest] + shift) % drawn.shape[longest]
        spots.append(tuple(where))
    return drawn.at[spots[0]].set(smallest).at[spots[1]].set(top_value)


def levels(key, extent, cuts, low, top_value):
    factor_of = 1.0
    for position, shards_of in cuts:
        draws = jax.random.uniform(jax.random.fold_in(jax.random.fold_in(key, 6), position), (shards_of,), jnp.float32, low / len(cuts), top_value / len(cuts))
        factor_of = factor_of * jnp.repeat(jnp.exp(draws), extent[position] // shards_of).reshape((-1,) + (1,) * (len(extent) - 1 - position))
    return factor_of


def normal_values(own_key, shape, scale, most, cuts=(), kind=jnp.bfloat16):
    result = jax.random.normal(own_key, shape, jnp.float32) * scale
    if len(cuts) > 0:
        result = levels(own_key, shape, cuts, -0.22, 0.18) * result
    return jnp.clip(result, min=-most, max=most).astype(kind)


def setup_inputs(seed: int = 0) -> dict:
    keys = jax.random.split(jax.random.key(seed), 7)
    return {
        "fields": normal_values(keys[0], (GRIDS, SRC_TILES, TS, GCOLS), 1.0, 6.0, ((1, 128),)),
        "weights": normal_values(keys[1], (GRIDS, TARGET_TILES, MAXP, TS, TT), (TS * MAXP // 2) ** -0.5, 0.5, ((1, 128),)),
        "pair_slots": with_ends(jax.random.randint(keys[2], (GRIDS, TARGET_TILES, MAXP), 0, REQ), jax.random.fold_in(keys[2], 1), 0, REQ - 1).astype(jnp.int32),
        "pair_counts": with_ends(jax.random.randint(keys[3], (GRIDS, TARGET_TILES), 1, MAXP + 1), jax.random.fold_in(keys[3], 1), 1, MAXP).astype(jnp.int32),
        "requests": draw_requests(jax.random.fold_in(keys[6], 71), 0),
        "eofs": normal_values(keys[5], (EOFS, CELLS), CELLS ** -0.5, 0.0078125, ((1, 128),)),
    }


def reference(fields, weights, pair_slots, pair_counts, requests, eofs):
    device_total = N_LAT * N_LON

    def one_device(running, device):
        start = device * TILES_DEV
        tile_weights = lax.dynamic_slice_in_dim(weights, start, TILES_DEV, 1)
        tile_slots = lax.dynamic_slice_in_dim(pair_slots, start, TILES_DEV, 1)
        tile_counts = lax.dynamic_slice_in_dim(pair_counts, start, TILES_DEV, 1)
        basis = lax.dynamic_slice_in_dim(eofs, start * TT, TILES_DEV * TT, 1)
        wanted = lax.dynamic_index_in_dim(requests, device, 1, keepdims=False)
        pieces = []
        for grid_id in range(GRIDS):
            tile_ids = wanted[grid_id][tile_slots[grid_id]]
            blocks = fields[grid_id][tile_ids]
            live_slots = jnp.arange(MAXP, dtype=jnp.int32)[None, :] < tile_counts[grid_id][:, None]
            masked = jnp.where(live_slots[:, :, None, None], tile_weights[grid_id], jnp.zeros((), jnp.bfloat16))
            regridded = jnp.einsum('tpsx,tpsc->txc', masked.astype(jnp.float32), blocks.astype(jnp.float32))
            by_model = regridded.reshape(TILES_DEV, TT, MODELS_G, MONTHS)
            anomaly = (by_model - jnp.mean(by_model, axis=3, keepdims=True)).astype(jnp.bfloat16)
            anomaly = anomaly.reshape(TILES_DEV * TT, MODELS_G * MONTHS)
            pieces.append(jnp.dot(basis, anomaly, preferred_element_type=jnp.float32))
        return running + jnp.concatenate(pieces, axis=1), None

    initial = jnp.zeros((EOFS, GRIDS * MODELS_G * MONTHS), jnp.float32)
    total, unused = lax.scan(one_device, initial, jnp.arange(device_total, dtype=jnp.int32))
    return total
```

```python
import functools

import jax
import jax.numpy as jnp
from jax import lax
from jax.experimental import pallas as pl
from jax.experimental.pallas import tpu as pltpu
from jax.sharding import PartitionSpec as P

MESH = pl.DeviceIdType.MESH
GRIDS, TILES, PAIRS, TS, TT = 3, 32, 8, 32, 128
STILES, CAP, COLS, EOFS = 16, 8, 384, 200
N_LAT, N_LON = 4, 32
DEVS = N_LAT * N_LON
OWN = 9
MONTHS = 24
GROUPS = 8
F32 = jnp.float32
BF16 = jnp.bfloat16


def pick(value, table):
    out = jnp.int32(table[-1])
    for index, entry in enumerate(table[:-1]):
        out = jnp.where(value == index, jnp.int32(entry), out)
    return out


def body(
    sel, code, fields, weights, eofs, out,
    fld, send, halo, wv, ev, gv, lhs, av, ft, pv, tails, outbox, inbox,
    sem_f, sem_w, sem_e, halo_s, halo_r, x_sem, z_sem, rs_s, rs_r,
):
    lat = lax.axis_index("lat")
    lon = lax.axis_index("lon")
    me = lat * N_LON + lon
    x = lon // 8
    inner = lon % 8
    right = lax.rem(lon + 1, N_LON)
    left = lax.rem(lon + N_LON - 1, N_LON)

    def lon_peer(step):
        return lax.rem(x + step, 4) * 8 + inner

    def group_peer(step):
        return x * 8 + lax.rem(inner + step, 8)

    barrier = pltpu.get_barrier_semaphore()

    def greet(to_lat, to_lon):
        pl.semaphore_signal(barrier, inc=1, device_id=(to_lat, to_lon), device_id_type=MESH)

    for step in range(1, 8):
        greet(lat, group_peer(step))
    greet(lat, left)
    greet(lat, right)
    for step in range(1, 4):
        greet(lat, lon_peer(step))
        greet(lax.rem(lat + step, 4), lon)

    field_copy = pltpu.make_async_copy(fields, fld, sem_f)
    field_copy.start()

    def e_copy(c):
        return pltpu.make_async_copy(
            eofs.at[:, pl.ds(pl.multiple_of(c * 512, 512), 512)], ev.at[c], sem_e.at[c]
        )

    def w_copy(c):
        return pltpu.make_async_copy(
            weights.at[:, pl.ds(c * 4, 4)], wv.at[c], sem_w.at[c]
        )

    @pl.loop(0, GROUPS)
    def _(c):
        e_copy(c).start()
        w_copy(c).start()

    rows = lax.broadcasted_iota(jnp.int32, (192, 256), 0)

    @pl.loop(0, GRIDS * GROUPS)
    def _(i):
        hit = rows == code[i]
        lhs[i] = jnp.where(hit, 1.0, 0.0).astype(BF16)

    field_copy.wait()
    for g in range(GRIDS):
        for way in range(2):
            for r in range(CAP):
                tile = sel[(2 * way * GRIDS + g) * CAP + r]
                send[way, g, pl.ds(r * TS, TS), :] = fld[g * STILES + tile]
    pl.semaphore_wait(barrier, 15)

    def halo_copy(way, g):
        return pltpu.make_async_remote_copy(
            src_ref=send.at[way, g],
            dst_ref=halo.at[way, g],
            send_sem=halo_s.at[way, g],
            recv_sem=halo_r.at[way, g],
            device_id=(lat, right if way == 0 else left),
            device_id_type=MESH,
        )

    for g in range(GRIDS):
        halo_copy(0, g).start()
        halo_copy(1, g).start()
    for step in range(1, 4):
        pl.semaphore_signal(x_sem, inc=1, device_id=(lat, lon_peer(step)), device_id_type=MESH)

    @pl.loop(0, GROUPS)
    def _(c):
        e_copy(c).wait()
        w_copy(c).wait()
        for tt in range(4):
            basis = ev[c, :, tt * TT : (tt + 1) * TT]
            for g in range(GRIDS):
                made = lax.dot_general(
                    wv[c, g, tt], basis, (((1,), (1,)), ((), ())), preferred_element_type=F32
                )
                wide = jnp.concatenate([made, jnp.zeros((256, 56), F32)], axis=1)
                gv[g, c, pl.ds(tt * 8, 8)] = wide.reshape(8, 4, 8, 256)

    pl.semaphore_wait(x_sem, 3)
    for step in range(1, 4):
        pl.semaphore_signal(
            z_sem, inc=1, device_id=(lax.rem(lat + step, 4), lon), device_id_type=MESH
        )

    for g in range(GRIDS):
        @pl.loop(0, 4)
        def _(q):
            total = jnp.zeros((192, 256), F32)
            for c in range(GROUPS):
                terms = gv[g, c, :, q].reshape(256, 256)
                high = terms.astype(BF16)
                low = (terms - high.astype(F32)).astype(BF16)
                chosen = lhs[g * GROUPS + c]
                total += jnp.dot(chosen, high, preferred_element_type=F32)
                total += jnp.dot(chosen, low, preferred_element_type=F32)
            av[g, :, q] = total.reshape(24, 8, 256)

    for g in range(GRIDS):
        own = jnp.concatenate(
            [fld[g * STILES + sel[(GRIDS + g) * CAP + r]] for r in range(CAP)], axis=0
        )
        ft[g] = own.T

    pl.semaphore_wait(z_sem, 3)

    for g in range(GRIDS):
        halo_copy(0, g).wait_recv()
        halo_copy(1, g).wait_recv()
        product = jnp.zeros((COLS, 256), F32)
        for part in range(3):
            source = av[g, pl.ds(part * CAP, CAP)].reshape(256, 256)
            high = source.astype(BF16)
            low = (source - high.astype(F32)).astype(BF16)
            turned = ft[g] if part == 1 else halo[part // 2, g].T
            product += jnp.dot(turned, high, preferred_element_type=F32)
            product += jnp.dot(turned, low, preferred_element_type=F32)
        by_model = product.reshape(COLS // MONTHS, MONTHS, 256)
        centred = by_model - jnp.sum(by_model, axis=1, keepdims=True) * (1.0 / MONTHS)
        centred = centred.reshape(COLS, 256)
        pv[0, pl.ds(g * COLS, COLS), :] = centred[:, :128]
        pv[1, pl.ds(g * COLS, COLS), :] = centred[:, 128:]

    lanes = lax.broadcasted_iota(jnp.int32, (8, 128), 1)

    @pl.loop(0, 16)
    def _(i):
        base = pl.multiple_of(i * 72, 8)
        last = [pv[half, pl.ds(base + 8, 8, stride=9), :] for half in range(2)]
        for r, (half, shift) in enumerate(((0, 72), (0, 16), (0, 88), (1, 72), (1, 16))):
            tails[i, pl.ds(r, 8, stride=8), :] = pltpu.roll(last[half], shift, 1)
        for r in range(5, 8):
            tails[i, pl.ds(r, 8, stride=8), :] = jnp.zeros((8, 128), F32)
        for j in range(8):
            first = pv[0, pl.ds(base + 9 * j, 8), :]
            second = jnp.where(
                lanes < 72, pv[1, pl.ds(base + 9 * j, 8), :], tails[i, 8 * j : 8 * j + 8, :]
            )
            outbox[i * 8 + j] = jnp.concatenate([first, second], axis=0).astype(BF16)

    def owner_copy(to_lat, to_lon):
        return pltpu.make_async_remote_copy(
            src_ref=outbox.at[to_lat * N_LON + to_lon],
            dst_ref=inbox.at[me],
            send_sem=rs_s,
            recv_sem=rs_r,
            device_id=(to_lat, to_lon),
            device_id_type=MESH,
        )

    order = (2, 1, 3, 0)

    @pl.loop(0, DEVS - 1)
    def _(i):
        to_lat = lax.rem(lat + pick(i // 32, order), 4)
        to_x = lax.rem(x + pick(lax.rem(i // 8, 4), order), 4)
        to_y = lax.rem(inner // 2 + pick(lax.rem(i // 2, 4), order), 4)
        to_core = lax.rem(inner + 1 + i, 2)
        owner_copy(to_lat, to_x * 8 + to_y * 2 + to_core).start()

    inbox[me] = outbox[me]
    everything = pltpu.make_async_remote_copy(
        src_ref=outbox.at[pl.ds(0, DEVS - 1)],
        dst_ref=inbox.at[pl.ds(0, DEVS - 1)],
        send_sem=rs_s,
        recv_sem=rs_r,
        device_id=(lat, right),
        device_id_type=MESH,
    )
    everything.wait_recv()
    total = jnp.zeros((16, 128), F32)
    for i in range(DEVS):
        total += inbox[i].astype(F32)
    out[...] = total

    everything.wait_send()
    for g in range(GRIDS):
        halo_copy(0, g).wait_send()
        halo_copy(1, g).wait_send()


def tables(pair_slots, pair_counts, requests):
    lat = lax.axis_index("lat")
    lon = lax.axis_index("lon")
    me = lat * N_LON + lon
    left = lat * N_LON + (lon + N_LON - 1) % N_LON
    right = lat * N_LON + (lon + 1) % N_LON
    row = lambda d: lax.dynamic_index_in_dim(requests, d, 1, keepdims=False)
    wanted = jnp.stack([row(right), row(me), row(left)])
    count = wanted.shape[-1]
    slots = jnp.arange(count, dtype=jnp.int32)
    earlier = slots[None, :] < slots[:, None]
    owner = wanted // STILES
    rank = jnp.sum(((owner[..., :, None] == owner[..., None, :]) & earlier).astype(jnp.int32), axis=-1)
    mine = (owner == me)[..., None] & (rank[..., None] == jnp.arange(CAP, dtype=jnp.int32))
    sel = jnp.sum(jnp.where(mine, (wanted % STILES)[..., None], 0), axis=2)
    own = owner[1]
    place = jnp.where(own == left, 0, jnp.where(own == me, CAP, 2 * CAP)) + rank[1]
    flat = pair_slots.reshape(GRIDS, TILES * PAIRS)
    position = jnp.sum(jnp.where(flat[..., None] == slots, place[:, None, :], 0), axis=-1)
    live = (jnp.arange(PAIRS, dtype=jnp.int32) < pair_counts[..., None]).reshape(GRIDS, TILES * PAIRS)
    eight = jnp.arange(8, dtype=jnp.int32)
    code = jnp.where(live, position * 8, -8)[..., None] + eight
    return sel.reshape(-1), code.reshape(GRIDS * GROUPS, 1, 256)


def shards(fields, weights, pair_slots, pair_counts, requests, eofs):
    sel, code = tables(pair_slots, pair_counts, requests)
    anywhere = pl.BlockSpec(memory_space=pl.ANY)
    summed = pl.pallas_call(
        body,
        out_shape=jax.ShapeDtypeStruct((16, 128), F32),
        in_specs=[
            pl.BlockSpec(memory_space=pltpu.SMEM),
            pl.BlockSpec(memory_space=pltpu.VMEM),
            anywhere,
            anywhere,
            anywhere,
        ],
        out_specs=pl.BlockSpec(memory_space=pltpu.VMEM),
        scratch_shapes=[
            pltpu.VMEM((GRIDS * STILES, TS, COLS), BF16),
            pltpu.VMEM((2, GRIDS, CAP * TS, COLS), BF16),
            pltpu.VMEM((2, GRIDS, CAP * TS, COLS), BF16),
            pltpu.VMEM((GROUPS, GRIDS, 4, 256, TT), BF16),
            pltpu.VMEM((GROUPS, EOFS, 512), BF16),
            pltpu.VMEM((GRIDS, GROUPS, 32, 4, 8, 256), F32),
            pltpu.VMEM((GRIDS * GROUPS, 192, 256), BF16),
            pltpu.VMEM((GRIDS, 24, 4, 8, 256), F32),
            pltpu.VMEM((GRIDS, COLS, 256), BF16),
            pltpu.VMEM((2, GRIDS * COLS + 8, 128), F32),
            pltpu.VMEM((16, 64, 128), F32),
            pltpu.VMEM((DEVS, 16, 128), BF16),
            pltpu.VMEM((DEVS, 16, 128), BF16),
            pltpu.SemaphoreType.DMA,
            pltpu.SemaphoreType.DMA((GROUPS,)),
            pltpu.SemaphoreType.DMA((GROUPS,)),
            pltpu.SemaphoreType.DMA((2, GRIDS)),
            pltpu.SemaphoreType.DMA((2, GRIDS)),
            pltpu.SemaphoreType.REGULAR,
            pltpu.SemaphoreType.REGULAR,
            pltpu.SemaphoreType.DMA,
            pltpu.SemaphoreType.DMA,
        ],
        compiler_params=pltpu.CompilerParams(
            collective_id=0, has_side_effects=True, vmem_limit_bytes=56 * 1024 * 1024
        ),
    )(
        sel,
        code,
        fields.reshape(GRIDS * STILES, TS, COLS),
        weights.reshape(GRIDS, TILES, PAIRS * TS, TT),
        eofs,
    )
    last = jnp.concatenate(
        [summed[8, 72:], summed[9, 72:], summed[10, 72:88], summed[11, 72:], summed[12, 72:88]]
    )
    first = jnp.concatenate([summed[:8], summed[8:, :72]], axis=1)
    return jnp.concatenate([first, last[None]], axis=0).T


def solution(mesh):
    return jax.shard_map(
        shards,
        mesh=mesh,
        in_specs=(
            P(None, ("lat", "lon"), None, None),
            P(None, ("lat", "lon"), None, None, None),
            P(None, ("lat", "lon"), None),
            P(None, ("lat", "lon")),
            P(),
            P(None, ("lat", "lon")),
        ),
        out_specs=P(None, ("lat", "lon")),
        check_vma=False,
    )
```

```python
import jax
import jax.numpy as jnp
from jax import lax
from jax.experimental import pallas as pl
from jax.experimental.pallas import tpu as pltpu
from jax.sharding import PartitionSpec as P

MESH = pl.DeviceIdType.MESH
GRIDS, TILES, PAIRS, TS, TT = 3, 32, 8, 32, 128
STILES, REQ, CAP, COLS, EOFS = 16, 16, 8, 384, 200
N_LAT, N_LON = 4, 32
DEVS = N_LAT * N_LON
OWN = 9
MONTHS = 24
GROUPS = 8
F32 = jnp.float32
BF16 = jnp.bfloat16
PHASES = ((0, 5), (5, 10), (10, 16))


def body(
    requests, slots, counts, fields, weights, eofs, out,
    wanted, slot_v, count_v, fld, send, halo_0, halo_1, halo_2, wv, ev, gv, lhs, av, pv, tails,
    outbox, inbox,
    sem_i, sem_f, sem_w, sem_e, halo_s, halo_r, x_sem, z_sem, rs_s, rs_r,
):
    lat = lax.axis_index("lat")
    lon = lax.axis_index("lon")
    me = lat * N_LON + lon
    right = (lon + 1) & 31
    left = (lon + 31) & 31
    halos = (halo_0, halo_1, halo_2)

    barrier = pltpu.get_barrier_semaphore()

    def greet(sem, to_lat, to_lon):
        pl.semaphore_signal(sem, inc=1, device_id=(to_lat, to_lon), device_id_type=MESH)

    with jax.named_scope("greet"):
        greet(barrier, lat, left)
        greet(barrier, lat, right)
        for step in range(1, 8):
            greet(barrier, lat, lon ^ step)
        for step in range(1, 4):
            greet(barrier, lat, lon ^ (step * 8))
            greet(barrier, lat ^ step, lon)

        inputs = [
            pltpu.make_async_copy(requests, wanted, sem_i.at[0]),
            pltpu.make_async_copy(slots, slot_v, sem_i.at[1]),
            pltpu.make_async_copy(counts, count_v, sem_i.at[2]),
        ]
        for copy in inputs:
            copy.start()
        field_copy = pltpu.make_async_copy(fields, fld, sem_f)
        field_copy.start()

    def e_copy(c):
        return pltpu.make_async_copy(
            eofs.at[:, pl.ds(pl.multiple_of(c * 512, 512), 512)], ev.at[c], sem_e.at[c]
        )

    def w_copy(c):
        return pltpu.make_async_copy(weights.at[:, pl.ds(c * 4, 4)], wv.at[c], sem_w.at[c])

    @pl.loop(0, GROUPS)
    def _(c):
        e_copy(c).start()
        w_copy(c).start()

    with jax.named_scope("codes"):
        inputs[1].wait()
        inputs[2].wait()
        live = lax.broadcasted_iota(jnp.int32, (GRIDS, PAIRS, TILES), 1) < count_v[...][:, None, :]
        marked = jnp.where(live, slot_v[...] + 1, 0).astype(F32)
        marked = marked.reshape(GRIDS * PAIRS, TILES).astype(BF16)
        lane = lax.broadcasted_iota(jnp.int32, (TILES, TILES * 64), 1)
        tile = lax.broadcasted_iota(jnp.int32, (TILES, TILES * 64), 0)
        spread = jnp.where((lane >> 6) == tile, 1.0, 0.0).astype(BF16)
        codes = jnp.dot(marked, spread, preferred_element_type=F32)
        codes = codes.reshape(GRIDS, PAIRS, TILES * 64)
        lane = lax.broadcasted_iota(jnp.int32, (PAIRS, TILES * 64), 1)
        pair = lax.broadcasted_iota(jnp.int32, (PAIRS, TILES * 64), 0)
        codes = jnp.sum(jnp.where(((lane >> 3) & 7) == pair, codes, 0.0), axis=1)
        row = (lax.broadcasted_iota(jnp.int32, (GRIDS, TILES * 64), 1) & 7).astype(F32)
        codes = codes * 8.0 + (row - 8.0)
        rows = lax.broadcasted_iota(jnp.int32, (128, 256), 0).astype(F32)
        for g in range(GRIDS):
            for c in range(GROUPS):
                hit = rows == codes[g : g + 1, c * 256 : (c + 1) * 256]
                lhs[g * GROUPS + c] = jnp.where(hit, 1.0, 0.0).astype(BF16)

    with jax.named_scope("pick"):
        inputs[0].wait()

        def mine_of(g, device):
            chosen = [jnp.int32(0)] * CAP
            seen = jnp.int32(0)
            for j in range(REQ):
                source = wanted[g * REQ + j, device]
                mine = (source >> 4) == me
                for r in range(min(j + 1, CAP)):
                    chosen[r] = jnp.where(mine & (seen == r), source & 15, chosen[r])
                seen = seen + jnp.where(mine, 1, 0)
            return chosen

        picked = [[mine_of(g, lat * N_LON + to) for g in range(GRIDS)] for to in (right, left)]

    with jax.named_scope("gather"):
        field_copy.wait()
        for g in range(GRIDS):
            for way in range(2):
                for r in range(CAP):
                    send[way, g, r] = fld[g * STILES + picked[way][g][r]]

    def halo_copy(way, g):
        return pltpu.make_async_remote_copy(
            src_ref=send.at[way, g],
            dst_ref=halos[g].at[way],
            send_sem=halo_s.at[way, g],
            recv_sem=halo_r.at[way, g],
            device_id=(lat, right if way == 0 else left),
            device_id_type=MESH,
        )

    def project(c):
        e_copy(c).wait()
        w_copy(c).wait()
        for tt in range(4):
            basis = ev[c, :, tt * TT : (tt + 1) * TT]
            for g in range(GRIDS):
                made = lax.dot_general(
                    wv[c, g, tt], basis, (((1,), (1,)), ((), ())), preferred_element_type=F32
                )
                wide = jnp.concatenate([made, jnp.zeros((256, 56), F32)], axis=1)
                gv[g, c, pl.ds(tt * 8, 8)] = wide.reshape(8, 4, 8, 256)

    with jax.named_scope("barrier"):
        pl.semaphore_wait(barrier, 15)
        for g in range(GRIDS):
            halo_copy(0, g).start()
            halo_copy(1, g).start()
        for step in range(1, 4):
            greet(x_sem, lat, lon ^ (step * 8))

    with jax.named_scope("project"):

        @pl.loop(0, GROUPS)
        def _(c):
            project(c)

    with jax.named_scope("barrier2"):
        pl.semaphore_wait(x_sem, 3)
        for step in range(1, 4):
            greet(z_sem, lat ^ step, lon)

    with jax.named_scope("addup"):
        for g in range(GRIDS):

            @pl.loop(0, 4)
            def _(q):
                total = jnp.zeros((128, 256), F32)
                for c in range(GROUPS):
                    terms = gv[g, c, :, q].reshape(256, 256)
                    high = terms.astype(BF16)
                    low = (terms - high.astype(F32)).astype(BF16)
                    chosen = lhs[g * GROUPS + c]
                    total += jnp.dot(chosen, high, preferred_element_type=F32)
                    total += jnp.dot(chosen, low, preferred_element_type=F32)
                av[g, :, q] = total.reshape(REQ, 8, 256)

    with jax.named_scope("barrier3"):
        pl.semaphore_wait(z_sem, 3)

    lanes = lax.broadcasted_iota(jnp.int32, (8, 128), 1)

    def owner_copy(owner):
        return pltpu.make_async_remote_copy(
            src_ref=outbox.at[owner],
            dst_ref=inbox.at[me],
            send_sem=rs_s,
            recv_sem=rs_r,
            device_id=(owner >> 5, owner & 31),
            device_id_type=MESH,
        )

    for g in range(GRIDS):
        with jax.named_scope(f"halo{g}"):
            halo_copy(0, g).wait_recv()
            halo_copy(1, g).wait_recv()
        with jax.named_scope(f"product{g}"):
            product = jnp.zeros((COLS, 256), F32)
            seen_left = jnp.int32(0)
            seen_right = jnp.int32(0)
            for half in range(2):
                blocks = []
                for j in range(half * 8, half * 8 + 8):
                    source = wanted[g * REQ + j, me]
                    owner = source >> 4
                    on_left = owner == lat * N_LON + left
                    on_me = owner == me
                    from_left = halos[g][0, seen_left & 7]
                    from_right = halos[g][1, seen_right & 7]
                    from_me = fld[g * STILES + (source & 15)]
                    blocks.append(
                        jnp.where(on_me, from_me, jnp.where(on_left, from_left, from_right))
                    )
                    seen_left = seen_left + jnp.where(on_left, 1, 0)
                    seen_right = seen_right + jnp.where(on_left | on_me, 0, 1)
                turned = jnp.concatenate(blocks, axis=0).T
                source = av[g, pl.ds(half * 8, 8)].reshape(256, 256)
                high = source.astype(BF16)
                low = (source - high.astype(F32)).astype(BF16)
                product += jnp.dot(turned, high, preferred_element_type=F32)
                product += jnp.dot(turned, low, preferred_element_type=F32)
            by_model = product.reshape(COLS // MONTHS, MONTHS, 256)
            centred = by_model - jnp.sum(by_model, axis=1, keepdims=True) * (1.0 / MONTHS)
            centred = centred.reshape(COLS, 256)
            pv[0, pl.ds(g * COLS, COLS), :] = centred[:, :128]
            pv[1, pl.ds(g * COLS, COLS), :] = centred[:, 128:]

        start, stop = PHASES[g]
        with jax.named_scope(f"pack{g}"):

            @pl.loop(start, stop)
            def _(i):
                base = pl.multiple_of(i * 72, 8)
                last = [pv[half, pl.ds(base + 8, 8, stride=9), :] for half in range(2)]
                for r, (half, shift) in enumerate(((0, 72), (0, 16), (0, 88), (1, 72), (1, 16))):
                    tails[i, pl.ds(r, 8, stride=8), :] = pltpu.roll(last[half], shift, 1)
                for r in range(5, 8):
                    tails[i, pl.ds(r, 8, stride=8), :] = jnp.zeros((8, 128), F32)
                for j in range(8):
                    first = pv[0, pl.ds(base + 9 * j, 8), :]
                    second = jnp.where(
                        lanes < 72, pv[1, pl.ds(base + 9 * j, 8), :], tails[i, 8 * j : 8 * j + 8, :]
                    )
                    outbox[i * 8 + j] = jnp.concatenate([first, second], axis=0).astype(BF16)

        with jax.named_scope(f"send{g}"):
            count = stop - start
            turn = lax.rem(me >> 3, count)

            @pl.loop(0, count)
            def _(k):
                group = k + turn
                group = start + group - jnp.where(group >= count, count, 0)

                @pl.when(group != me >> 3)
                def _():
                    owner_copy(group * 8 + (me & 7)).start()

                for j in range(1, 8):
                    owner_copy(group * 8 + ((me & 7) ^ j)).start()

    with jax.named_scope("arrive"):
        inbox[me] = outbox[me]
        everything = pltpu.make_async_remote_copy(
            src_ref=outbox.at[pl.ds(0, DEVS - 1)],
            dst_ref=inbox.at[pl.ds(0, DEVS - 1)],
            send_sem=rs_s,
            recv_sem=rs_r,
            device_id=(lat, right),
            device_id_type=MESH,
        )
        everything.wait_recv()
    with jax.named_scope("final"):
        total = jnp.zeros((16, 128), F32)
        for i in range(DEVS):
            total += inbox[i].astype(F32)
        first, second = total[:8], total[8:]
        by_56, by_112, by_40 = (pltpu.roll(second, shift, 1) for shift in (56, 112, 40))
        lane = lanes[:1]
        last_0 = jnp.where(lane < 56, by_56[0:1], jnp.where(lane < 112, by_112[1:2], by_40[2:3]))
        last_1 = jnp.where(lane < 56, by_56[3:4], by_112[4:5])
        out[0:8, 0:128] = first
        out[0:8, 128:EOFS] = second[:, : EOFS - 128]
        out[8:9, 0:128] = last_0
        out[8:9, 128:EOFS] = last_1[:, : EOFS - 128]

    with jax.named_scope("drain"):
        everything.wait_send()
        for g in range(GRIDS):
            halo_copy(0, g).wait_send()
            halo_copy(1, g).wait_send()


def shards(fields, weights, pair_slots, pair_counts, requests, eofs):
    return pl.pallas_call(
        body,
        out_shape=jax.ShapeDtypeStruct((OWN, EOFS), F32),
        in_specs=[pl.BlockSpec(memory_space=pl.ANY)] * 6,
        out_specs=pl.BlockSpec(memory_space=pltpu.VMEM),
        scratch_shapes=[
            pltpu.SMEM((GRIDS * REQ, DEVS), jnp.int32),
            pltpu.VMEM((GRIDS, PAIRS, TILES), jnp.int32),
            pltpu.VMEM((GRIDS, TILES), jnp.int32),
            pltpu.VMEM((GRIDS * STILES, TS, COLS), BF16),
            pltpu.VMEM((2, GRIDS, CAP, TS, COLS), BF16),
            pltpu.VMEM((2, CAP, TS, COLS), BF16),
            pltpu.VMEM((2, CAP, TS, COLS), BF16),
            pltpu.VMEM((2, CAP, TS, COLS), BF16),
            pltpu.VMEM((GROUPS, GRIDS, 4, 256, TT), BF16),
            pltpu.VMEM((GROUPS, EOFS, 512), BF16),
            pltpu.VMEM((GRIDS, GROUPS, 32, 4, 8, 256), F32),
            pltpu.VMEM((GRIDS * GROUPS, 128, 256), BF16),
            pltpu.VMEM((GRIDS, REQ, 4, 8, 256), F32),
            pltpu.VMEM((2, GRIDS * COLS + 8, 128), F32),
            pltpu.VMEM((16, 64, 128), F32),
            pltpu.VMEM((DEVS, 16, 128), BF16),
            pltpu.VMEM((DEVS, 16, 128), BF16),
            pltpu.SemaphoreType.DMA((3,)),
            pltpu.SemaphoreType.DMA,
            pltpu.SemaphoreType.DMA((GROUPS,)),
            pltpu.SemaphoreType.DMA((GROUPS,)),
            pltpu.SemaphoreType.DMA((2, GRIDS)),
            pltpu.SemaphoreType.DMA((2, GRIDS)),
            pltpu.SemaphoreType.REGULAR,
            pltpu.SemaphoreType.REGULAR,
            pltpu.SemaphoreType.DMA,
            pltpu.SemaphoreType.DMA,
        ],
        compiler_params=pltpu.CompilerParams(
            collective_id=0, has_side_effects=True, vmem_limit_bytes=56 * 1024 * 1024
        ),
    )(
        requests.transpose(0, 2, 1).reshape(GRIDS * REQ, DEVS),
        pair_slots.transpose(0, 2, 1),
        pair_counts,
        fields.reshape(GRIDS * STILES, TS, COLS),
        weights.reshape(GRIDS, TILES, PAIRS * TS, TT),
        eofs,
    ).T


def solution(mesh):
    return jax.shard_map(
        shards,
        mesh=mesh,
        in_specs=(
            P(None, ("lat", "lon"), None, None),
            P(None, ("lat", "lon"), None, None, None),
            P(None, ("lat", "lon"), None),
            P(None, ("lat", "lon")),
            P(),
            P(None, ("lat", "lon")),
        ),
        out_specs=P(None, ("lat", "lon")),
        check_vma=False,
    )
```

```python
import jax
import jax.numpy as jnp
from jax import lax
from jax.experimental import pallas as pl
from jax.experimental.pallas import tpu as pltpu
from jax.sharding import PartitionSpec as P

MESH = pl.DeviceIdType.MESH
GRIDS, TILES, PAIRS, TS, TT = 3, 32, 8, 32, 128
STILES, REQ, CAP, COLS, EOFS = 16, 16, 8, 384, 200
N_LAT, N_LON = 4, 32
DEVS = N_LAT * N_LON
OWN = 9
MONTHS = 24
GROUPS = 8
SPLIT = 4
F32 = jnp.float32
BF16 = jnp.bfloat16
PHASES = ((0, 0, 5), (1, 5, 10), (2, 10, 16))
CHIPS = DEVS // 2


def body(
    requests, slots, counts, fields, weights, eofs, out,
    wanted, slot_v, count_v, fld, send, halo_0, halo_1, halo_2, wv, ev, gv, lhs, av, pv, tails,
    pairbox, twinbox, outbox, inbox,
    sem_i, sem_f, sem_w, sem_e, halo_s, halo_r, x_sem, z_sem, pair_s, pair_r, rs_s, rs_r,
):
    lat = lax.axis_index("lat")
    lon = lax.axis_index("lon")
    me = lat * N_LON + lon
    core = lon & 1
    chip = me >> 1
    right = (lon + 1) & 31
    left = (lon + 31) & 31
    halos = (halo_0, halo_1, halo_2)

    barrier = pltpu.get_barrier_semaphore()

    def greet(sem, to_lat, to_lon):
        pl.semaphore_signal(sem, inc=1, device_id=(to_lat, to_lon), device_id_type=MESH)

    with jax.named_scope("greet"):
        greet(barrier, lat, left)
        greet(barrier, lat, right)
        for step in range(1, 8):
            greet(barrier, lat, lon ^ step)
        for step in range(1, 4):
            greet(barrier, lat, lon ^ (step * 8))
            greet(barrier, lat ^ step, lon)

        inputs = [
            pltpu.make_async_copy(requests, wanted, sem_i.at[0]),
            pltpu.make_async_copy(slots, slot_v, sem_i.at[1]),
            pltpu.make_async_copy(counts, count_v, sem_i.at[2]),
        ]
        for copy in inputs:
            copy.start()
        field_copy = pltpu.make_async_copy(fields, fld, sem_f)
        field_copy.start()

    def e_copy(c):
        return pltpu.make_async_copy(
            eofs.at[:, pl.ds(pl.multiple_of(c * 512, 512), 512)], ev.at[c, pl.ds(0, EOFS)], sem_e.at[c]
        )

    def w_copy(c):
        return [
            pltpu.make_async_copy(weights.at[:, c * 4 + tt], wv.at[c, tt], sem_w.at[c, tt])
            for tt in range(4)
        ]

    @pl.loop(0, GROUPS)
    def _(c):
        ev[c, 192:256, :] = jnp.zeros((64, 512), BF16)
        e_copy(c).start()
        for copy in w_copy(c):
            copy.start()

    with jax.named_scope("inputs"):
        for copy in inputs:
            copy.wait()

    def mine_of(g, device):
        packed = jnp.int32(0)
        place = jnp.int32(1)
        for j in range(REQ):
            source = wanted[g * REQ + j, device]
            mine = (source >> 4) == me
            packed = packed + jnp.where(mine, (source & 15) * place, 0)
            place = jnp.where(mine, place * 16, place)
        return [lax.shift_right_logical(packed, jnp.int32(4 * r)) & 15 for r in range(CAP)]

    with jax.named_scope("pick"):
        picked = [[mine_of(g, lat * N_LON + to) for g in range(GRIDS)] for to in (right, left)]

    with jax.named_scope("gather"):
        with jax.named_scope("wait_f"):
            field_copy.wait()
        for g in range(GRIDS):
            for way in range(2):
                for r in range(CAP):
                    send[way, g, r] = fld[g * STILES + picked[way][g][r]]

    def halo_copy(way, g):
        return pltpu.make_async_remote_copy(
            src_ref=send.at[way, g],
            dst_ref=halos[g].at[way],
            send_sem=halo_s.at[way, g],
            recv_sem=halo_r.at[way, g],
            device_id=(lat, right if way == 0 else left),
            device_id_type=MESH,
        )

    def project(c):
        rows = lax.broadcasted_iota(jnp.int32, (128, 256), 0).astype(F32)
        for g in range(GRIDS):
            hit = rows == codes[g : g + 1, c * 256 : (c + 1) * 256]
            lhs[g * GROUPS + c] = jnp.where(hit, 1.0, 0.0).astype(BF16)
        for tt in range(4):
            basis = ev[c, :, tt * TT : (tt + 1) * TT]
            made = lax.dot_general(
                wv[c, tt].reshape(GRIDS * 256, TT), basis, (((1,), (1,)), ((), ())),
                preferred_element_type=F32,
            )
            wide = made.reshape(GRIDS, 8, 4, 8, 256)
            for g in range(GRIDS):
                for q in range(4):
                    gv[g, c, q, pl.ds(tt * 8, 8)] = wide[g, :, q]

    def arrived(c):
        e_copy(c).wait()
        for copy in w_copy(c):
            copy.wait()

    with jax.named_scope("barrier"):
        pl.semaphore_wait(barrier, 15)
        for g, _, _ in PHASES:
            halo_copy(0, g).start()
            halo_copy(1, g).start()
        for step in range(1, 4):
            greet(x_sem, lat, lon ^ (step * 8))

    with jax.named_scope("wait_a"):
        for c in range(SPLIT):
            arrived(c)

    with jax.named_scope("project_a"):
        live = lax.broadcasted_iota(jnp.int32, (GRIDS, PAIRS, TILES), 1) < count_v[...][:, None, :]
        marked = jnp.where(live, slot_v[...] + 1, 0).astype(F32)
        marked = marked.reshape(GRIDS * PAIRS, TILES).astype(BF16)
        lane = lax.broadcasted_iota(jnp.int32, (TILES, TILES * 64), 1)
        tile = lax.broadcasted_iota(jnp.int32, (TILES, TILES * 64), 0)
        spread = jnp.where((lane >> 6) == tile, 1.0, 0.0).astype(BF16)
        codes = jnp.dot(marked, spread, preferred_element_type=F32)
        codes = codes.reshape(GRIDS, PAIRS, TILES * 64)
        lane = lax.broadcasted_iota(jnp.int32, (PAIRS, TILES * 64), 1)
        pair = lax.broadcasted_iota(jnp.int32, (PAIRS, TILES * 64), 0)
        codes = jnp.sum(jnp.where(((lane >> 3) & 7) == pair, codes, 0.0), axis=1)
        row = (lax.broadcasted_iota(jnp.int32, (GRIDS, TILES * 64), 1) & 7).astype(F32)
        codes = codes * 8.0 + (row - 8.0)
        for c in range(SPLIT):
            project(c)

    with jax.named_scope("barrier2"):
        pl.semaphore_wait(x_sem, 3)
        for step in range(1, 4):
            greet(z_sem, lat ^ step, lon)

    with jax.named_scope("wait_b"):
        for c in range(SPLIT, GROUPS):
            arrived(c)

    with jax.named_scope("project_b"):
        for c in range(SPLIT, GROUPS):
            project(c)

    lanes = lax.broadcasted_iota(jnp.int32, (8, 128), 1)

    def pair_copy(turn):
        _, start, stop = PHASES[turn]
        return pltpu.make_async_remote_copy(
            src_ref=pairbox.at[1 - core, pl.ds(start * 4, (stop - start) * 4)],
            dst_ref=twinbox.at[pl.ds(start * 4, (stop - start) * 4)],
            send_sem=pair_s.at[turn],
            recv_sem=pair_r.at[turn],
            device_id=(lat, lon ^ 1),
            device_id_type=MESH,
        )

    def owner_copy(place, to_core, slot):
        owner = place * 2 + to_core
        return pltpu.make_async_remote_copy(
            src_ref=outbox.at[place],
            dst_ref=inbox.at[slot],
            send_sem=rs_s,
            recv_sem=rs_r,
            device_id=(owner >> 5, owner & 31),
            device_id_type=MESH,
        )

    def deliver(turn):
        _, start, stop = PHASES[turn]
        count = stop - start
        with jax.named_scope(f"pair{turn}"):
            pair_copy(turn).wait_recv()
            if turn == 0:
                pl.semaphore_wait(z_sem, 3)
        with jax.named_scope(f"send{turn}"):
            for i in range(start * 4, stop * 4):
                outbox[i] = (pairbox[core, i] + twinbox[i]).astype(BF16)
            first_group = lax.rem(chip >> 2, count)
            for k in range(count):
                group = k + first_group
                group = start + group - jnp.where(group >= count, count, 0)
                own = group == chip >> 2
                place = group * 4 + (chip & 3)
                owner_copy(
                    place, jnp.where(own, 1 - core, core), jnp.where(own, CHIPS, chip)
                ).start()
                for j in range(1, 4):
                    owner_copy(group * 4 + ((chip & 3) ^ j), core, chip).start()

    def landed(g):
        with jax.named_scope(f"halo{g}"):
            halo_copy(0, g).wait_recv()
            halo_copy(1, g).wait_recv()

    for turn, (g, start, stop) in enumerate(PHASES):
        if turn > 0:
            landed(g)
        with jax.named_scope(f"addup{g}"):

            @pl.loop(0, 4, unroll=True)
            def _(q):
                total = jnp.zeros((128, 256), F32)
                for c in range(GROUPS):
                    terms = gv[g, c, q].reshape(256, 256)
                    high = terms.astype(BF16)
                    low = (terms - high.astype(F32)).astype(BF16)
                    chosen = lhs[g * GROUPS + c]
                    total += jnp.dot(chosen, high, preferred_element_type=F32)
                    total += jnp.dot(chosen, low, preferred_element_type=F32)
                av[g, :, q] = total.reshape(REQ, 8, 256)

        if turn == 0:
            landed(g)
        if turn > 0:
            deliver(turn - 1)
        with jax.named_scope(f"product{g}"):
            product = jnp.zeros((COLS, 256), F32)
            seen_left = jnp.int32(0)
            seen_right = jnp.int32(0)
            for half in range(2):
                blocks = []
                for j in range(half * 8, half * 8 + 8):
                    source = wanted[g * REQ + j, me]
                    owner = source >> 4
                    on_left = owner == lat * N_LON + left
                    on_me = owner == me
                    from_left = halos[g][0, seen_left & 7]
                    from_right = halos[g][1, seen_right & 7]
                    from_me = fld[g * STILES + (source & 15)]
                    blocks.append(
                        jnp.where(on_me, from_me, jnp.where(on_left, from_left, from_right))
                    )
                    seen_left = seen_left + jnp.where(on_left, 1, 0)
                    seen_right = seen_right + jnp.where(on_left | on_me, 0, 1)
                turned = jnp.concatenate(blocks, axis=0).T
                source = av[g, pl.ds(half * 8, 8)].reshape(256, 256)
                high = source.astype(BF16)
                low = (source - high.astype(F32)).astype(BF16)
                product += jnp.dot(turned, high, preferred_element_type=F32)
                product += jnp.dot(turned, low, preferred_element_type=F32)
            by_model = product.reshape(COLS // MONTHS, MONTHS, 256)
            centred = by_model - jnp.sum(by_model, axis=1, keepdims=True) * (1.0 / MONTHS)
            centred = centred.reshape(COLS, 256)
            pv[0, pl.ds(g * COLS, COLS), :] = centred[:, :128]
            pv[1, pl.ds(g * COLS, COLS), :] = centred[:, 128:]

        with jax.named_scope(f"pack{g}"):

            @pl.loop(start, stop, unroll=True)
            def _(i):
                base = pl.multiple_of(i * 72, 8)
                last = [pv[half, pl.ds(base + 8, 8, stride=9), :] for half in range(2)]
                for r, (half, shift) in enumerate(((0, 72), (0, 16), (0, 88), (1, 72), (1, 16))):
                    tails[i, pl.ds(r, 8, stride=8), :] = pltpu.roll(last[half], shift, 1)
                for r in range(5, 8):
                    tails[i, pl.ds(r, 8, stride=8), :] = jnp.zeros((8, 128), F32)
                for j in range(8):
                    first = pv[0, pl.ds(base + 9 * j, 8), :]
                    second = jnp.where(
                        lanes < 72, pv[1, pl.ds(base + 9 * j, 8), :], tails[i, 8 * j : 8 * j + 8, :]
                    )
                    pairbox[j & 1, i * 4 + j // 2] = jnp.concatenate([first, second], axis=0)

            pair_copy(turn).start()

    deliver(GRIDS - 1)

    with jax.named_scope("arrive"):
        inbox[chip] = outbox[chip]
        everything = pltpu.make_async_remote_copy(
            src_ref=outbox,
            dst_ref=inbox.at[pl.ds(0, CHIPS)],
            send_sem=rs_s,
            recv_sem=rs_r,
            device_id=(lat, right),
            device_id_type=MESH,
        )
        everything.wait_recv()
    with jax.named_scope("final"):
        total = jnp.zeros((16, 128), F32)
        for i in range(CHIPS):
            total += inbox[i].astype(F32)
        first, second = total[:8], total[8:]
        by_56, by_112, by_40 = (pltpu.roll(second, shift, 1) for shift in (56, 112, 40))
        lane = lanes[:1]
        last_0 = jnp.where(lane < 56, by_56[0:1], jnp.where(lane < 112, by_112[1:2], by_40[2:3]))
        last_1 = jnp.where(lane < 56, by_56[3:4], by_112[4:5])
        out[0:8, 0:128] = first
        out[0:8, 128:EOFS] = second[:, : EOFS - 128]
        out[8:9, 0:128] = last_0
        out[8:9, 128:EOFS] = last_1[:, : EOFS - 128]

    with jax.named_scope("drain"):
        everything.wait_send()
        for g in range(GRIDS):
            halo_copy(0, g).wait_send()
            halo_copy(1, g).wait_send()
            pair_copy(g).wait_send()


def shards(fields, weights, pair_slots, pair_counts, requests, eofs):
    return pl.pallas_call(
        body,
        out_shape=pltpu.VMEM((OWN, EOFS), F32),
        in_specs=[pl.BlockSpec(memory_space=pl.ANY)] * 6,
        out_specs=pl.BlockSpec(memory_space=pltpu.VMEM),
        scratch_shapes=[
            pltpu.SMEM((GRIDS * REQ, DEVS), jnp.int32),
            pltpu.VMEM((GRIDS, PAIRS, TILES), jnp.int32),
            pltpu.VMEM((GRIDS, TILES), jnp.int32),
            pltpu.VMEM((GRIDS * STILES, TS, COLS), BF16),
            pltpu.VMEM((2, GRIDS, CAP, TS, COLS), BF16),
            pltpu.VMEM((2, CAP, TS, COLS), BF16),
            pltpu.VMEM((2, CAP, TS, COLS), BF16),
            pltpu.VMEM((2, CAP, TS, COLS), BF16),
            pltpu.VMEM((GROUPS, 4, GRIDS, 256, TT), BF16),
            pltpu.VMEM((GROUPS, 256, 512), BF16),
            pltpu.VMEM((GRIDS, GROUPS, 4, 32, 8, 256), F32),
            pltpu.VMEM((GRIDS * GROUPS, 128, 256), BF16),
            pltpu.VMEM((GRIDS, REQ, 4, 8, 256), F32),
            pltpu.VMEM((2, GRIDS * COLS + 8, 128), F32),
            pltpu.VMEM((16, 64, 128), F32),
            pltpu.VMEM((2, CHIPS, 16, 128), F32),
            pltpu.VMEM((CHIPS, 16, 128), F32),
            pltpu.VMEM((CHIPS, 16, 128), BF16),
            pltpu.VMEM((CHIPS + 1, 16, 128), BF16),
            pltpu.SemaphoreType.DMA((3,)),
            pltpu.SemaphoreType.DMA,
            pltpu.SemaphoreType.DMA((GROUPS, 4)),
            pltpu.SemaphoreType.DMA((GROUPS,)),
            pltpu.SemaphoreType.DMA((2, GRIDS)),
            pltpu.SemaphoreType.DMA((2, GRIDS)),
            pltpu.SemaphoreType.REGULAR,
            pltpu.SemaphoreType.REGULAR,
            pltpu.SemaphoreType.DMA((GRIDS,)),
            pltpu.SemaphoreType.DMA((GRIDS,)),
            pltpu.SemaphoreType.DMA,
            pltpu.SemaphoreType.DMA,
        ],
        compiler_params=pltpu.CompilerParams(
            collective_id=0, has_side_effects=True, vmem_limit_bytes=56 * 1024 * 1024
        ),
    )(
        requests.transpose(0, 2, 1).reshape(GRIDS * REQ, DEVS),
        pair_slots.transpose(0, 2, 1),
        pair_counts,
        fields.reshape(GRIDS * STILES, TS, COLS),
        weights.reshape(GRIDS, TILES, PAIRS * TS, TT),
        eofs,
    ).T


def solution(mesh):
    return jax.shard_map(
        shards,
        mesh=mesh,
        in_specs=(
            P(None, ("lat", "lon"), None, None),
            P(None, ("lat", "lon"), None, None, None),
            P(None, ("lat", "lon"), None),
            P(None, ("lat", "lon")),
            P(),
            P(None, ("lat", "lon")),
        ),
        out_specs=P(None, ("lat", "lon")),
        check_vma=False,
    )
```

```python
import jax
import jax.numpy as jnp
from jax import lax
from jax.experimental import pallas as pl
from jax.experimental.pallas import tpu as pltpu
from jax.sharding import PartitionSpec as P

MESH = pl.DeviceIdType.MESH
GRIDS, TILES, PAIRS, TS, TT = 3, 32, 8, 32, 128
STILES, REQ, CAP, COLS, EOFS = 16, 16, 8, 384, 200
N_LAT, N_LON = 4, 32
DEVS = N_LAT * N_LON
OWN = 9
MONTHS = 24
GROUPS = 8
HUB = 1
SPLIT = 4
F32 = jnp.float32
BF16 = jnp.bfloat16
PHASES = ((0, 0, 5), (1, 5, 10), (2, 10, 16))
CHIPS = DEVS // 2


def body(
    requests, slots, counts, fields, weights, eofs, out,
    wanted, slot_v, count_v, fld, send, halo_0, halo_1, halo_2, wv, ev, gv, lhs, av, pv, tails,
    pairbox, twinbox, outbox, inbox,
    sem_i, sem_f, sem_w, sem_e, halo_s, halo_r, x_sem, z_sem, g_sem, own_sem, pair_s, pair_r, rs_s, rs_r,
):
    lat = lax.axis_index("lat")
    lon = lax.axis_index("lon")
    me = lat * N_LON + lon
    core = lon & 1
    hub = (lon & 7) == HUB
    chip = me >> 1
    right = (lon + 1) & 31
    left = (lon + 31) & 31
    halos = (halo_0, halo_1, halo_2)

    def fence():
        pl.semaphore_signal(own_sem, inc=1)
        pl.semaphore_wait(own_sem, 1)

    barrier = pltpu.get_barrier_semaphore()

    def greet(sem, to_lat, to_lon):
        pl.semaphore_signal(sem, inc=1, device_id=(to_lat, to_lon), device_id_type=MESH)

    with jax.named_scope("greet"):
        greet(barrier, lat, left)
        greet(barrier, lat, right)
        for step in range(1, 8):
            greet(barrier, lat, lon ^ step)

        @pl.when(hub)
        def _():
            for step in range(1, 4):
                greet(barrier, lat, lon ^ (step * 8))
                greet(barrier, lat ^ step, lon)

        inputs = [
            pltpu.make_async_copy(requests, wanted, sem_i.at[0]),
            pltpu.make_async_copy(slots, slot_v, sem_i.at[1]),
            pltpu.make_async_copy(counts, count_v, sem_i.at[2]),
        ]
        for copy in inputs:
            copy.start()
        field_copy = pltpu.make_async_copy(fields, fld, sem_f)
        field_copy.start()

    def e_copy(c):
        return pltpu.make_async_copy(
            eofs.at[:, pl.ds(pl.multiple_of(c * 512, 512), 512)], ev.at[c, pl.ds(0, EOFS)], sem_e.at[c]
        )

    def w_copy(c):
        return [
            pltpu.make_async_copy(weights.at[:, c * 4 + tt], wv.at[c, tt], sem_w.at[c, tt])
            for tt in range(4)
        ]

    @pl.loop(0, GROUPS)
    def _(c):
        ev[c, 192:256, :] = jnp.zeros((64, 512), BF16)
        e_copy(c).start()
        for copy in w_copy(c):
            copy.start()

    with jax.named_scope("inputs"):
        for copy in inputs:
            copy.wait()

    def mine_of(g, device):
        packed = jnp.int32(0)
        place = jnp.int32(1)
        for j in range(REQ):
            source = wanted[g * REQ + j, device]
            mine = (source >> 4) == me
            packed = packed + jnp.where(mine, (source & 15) * place, 0)
            place = jnp.where(mine, place * 16, place)
        return [lax.shift_right_logical(packed, jnp.int32(4 * r)) & 15 for r in range(CAP)]

    with jax.named_scope("pick"):
        picked = [[mine_of(g, lat * N_LON + to) for g in range(GRIDS)] for to in (right, left)]

    with jax.named_scope("gather"):
        with jax.named_scope("wait_f"):
            field_copy.wait()
        for g in range(GRIDS):
            for way in range(2):
                for r in range(CAP):
                    send[way, g, r] = fld[g * STILES + picked[way][g][r]]

    def halo_copy(way, g):
        return pltpu.make_async_remote_copy(
            src_ref=send.at[way, g],
            dst_ref=halos[g].at[way],
            send_sem=halo_s.at[way, g],
            recv_sem=halo_r.at[way, g],
            device_id=(lat, right if way == 0 else left),
            device_id_type=MESH,
        )

    def project(c):
        rows = lax.broadcasted_iota(jnp.int32, (128, 256), 0).astype(F32)
        for g in range(GRIDS):
            hit = rows == codes[g : g + 1, c * 256 : (c + 1) * 256]
            lhs[g * GROUPS + c] = jnp.where(hit, 1.0, 0.0).astype(BF16)
        for tt in range(4):
            basis = ev[c, :, tt * TT : (tt + 1) * TT]
            made = lax.dot_general(
                wv[c, tt].reshape(GRIDS * 256, TT), basis, (((1,), (1,)), ((), ())),
                preferred_element_type=F32,
            )
            wide = made.reshape(GRIDS, 8, 4, 8, 256)
            for g in range(GRIDS):
                for q in range(4):
                    terms = wide[g, :, q].reshape(64, 256)
                    high = terms.astype(BF16)
                    gv[g, c, q, 0, pl.ds(tt * 64, 64), :] = high
                    gv[g, c, q, 1, pl.ds(tt * 64, 64), :] = (terms - high.astype(F32)).astype(BF16)

    def arrived(c):
        e_copy(c).wait()
        for copy in w_copy(c):
            copy.wait()

    with jax.named_scope("barrier"):
        pl.semaphore_wait(barrier, jnp.where(hub, 15, 9))
        for g, _, _ in PHASES:
            halo_copy(0, g).start()
            halo_copy(1, g).start()

        @pl.when(hub)
        def _():
            for step in range(1, 4):
                greet(x_sem, lat, lon ^ (step * 8))

    with jax.named_scope("wait_0"):
        for c in range(0, 2):
            arrived(c)

    with jax.named_scope("project_0"):
        live = lax.broadcasted_iota(jnp.int32, (GRIDS, PAIRS, TILES), 1) < count_v[...][:, None, :]
        marked = jnp.where(live, slot_v[...] + 1, 0).astype(F32)
        marked = marked.reshape(GRIDS * PAIRS, TILES).astype(BF16)
        lane = lax.broadcasted_iota(jnp.int32, (TILES, TILES * 64), 1)
        tile = lax.broadcasted_iota(jnp.int32, (TILES, TILES * 64), 0)
        spread = jnp.where((lane >> 6) == tile, 1.0, 0.0).astype(BF16)
        codes = jnp.dot(marked, spread, preferred_element_type=F32)
        codes = codes.reshape(GRIDS, PAIRS, TILES * 64)
        lane = lax.broadcasted_iota(jnp.int32, (PAIRS, TILES * 64), 1)
        pair = lax.broadcasted_iota(jnp.int32, (PAIRS, TILES * 64), 0)
        codes = jnp.sum(jnp.where(((lane >> 3) & 7) == pair, codes, 0.0), axis=1)
        row = (lax.broadcasted_iota(jnp.int32, (GRIDS, TILES * 64), 1) & 7).astype(F32)
        codes = codes * 8.0 + (row - 8.0)
        for c in range(0, 2):
            project(c)

    with jax.named_scope("barrier2"):

        @pl.when(hub)
        def _():
            pl.semaphore_wait(x_sem, 3)
            for step in range(1, 4):
                greet(z_sem, lat ^ step, lon)

    with jax.named_scope("wait_1"):
        for c in range(2, 5):
            arrived(c)

    with jax.named_scope("project_1"):
        for c in range(2, 5):
            project(c)

    with jax.named_scope("barrier3"):

        @pl.when(hub)
        def _():
            pl.semaphore_wait(z_sem, 3)
            for step in range(1, 8):
                greet(g_sem, lat, lon ^ step)

    with jax.named_scope("wait_2"):
        for c in range(5, 8):
            arrived(c)

    with jax.named_scope("project_2"):
        for c in range(5, 8):
            project(c)

    lanes = lax.broadcasted_iota(jnp.int32, (8, 128), 1)

    def pair_copy(turn):
        _, start, stop = PHASES[turn]
        return pltpu.make_async_remote_copy(
            src_ref=pairbox.at[1 - core, pl.ds(start * 4, (stop - start) * 4)],
            dst_ref=twinbox.at[pl.ds(start * 4, (stop - start) * 4)],
            send_sem=pair_s.at[turn],
            recv_sem=pair_r.at[turn],
            device_id=(lat, lon ^ 1),
            device_id_type=MESH,
        )

    def owner_copy(place, to_core, slot):
        owner = place * 2 + to_core
        return pltpu.make_async_remote_copy(
            src_ref=outbox.at[place],
            dst_ref=inbox.at[slot],
            send_sem=rs_s,
            recv_sem=rs_r,
            device_id=(owner >> 5, owner & 31),
            device_id_type=MESH,
        )

    def deliver(turn):
        _, start, stop = PHASES[turn]
        count = stop - start
        with jax.named_scope(f"pair{turn}"):
            pair_copy(turn).wait_recv()
            if turn == 0:

                @pl.when(jnp.logical_not(hub))
                def _():
                    pl.semaphore_wait(g_sem, 1)

        with jax.named_scope(f"send{turn}"):
            for i in range(start * 4, stop * 4):
                outbox[i] = (pairbox[core, i] + twinbox[i]).astype(BF16)
            first_group = lax.rem(chip >> 2, count)
            for k in range(count):
                group = k + first_group
                group = start + group - jnp.where(group >= count, count, 0)
                own = group == chip >> 2
                place = group * 4 + (chip & 3)
                owner_copy(
                    place, jnp.where(own, 1 - core, core), jnp.where(own, CHIPS, chip)
                ).start()
                for j in range(1, 4):
                    owner_copy(group * 4 + ((chip & 3) ^ j), core, chip).start()

    def landed(g):
        with jax.named_scope(f"halo{g}"):
            halo_copy(0, g).wait_recv()
            halo_copy(1, g).wait_recv()

    for turn, (g, start, stop) in enumerate(PHASES):
        with jax.named_scope(f"addup{g}"):
            fence()

            @pl.loop(0, 4, unroll=True)
            def _(q):
                total = jnp.zeros((128, 256), F32)
                for c in range(GROUPS):
                    chosen = lhs[g * GROUPS + c]
                    total += jnp.dot(chosen, gv[g, c, q, 0], preferred_element_type=F32)
                    total += jnp.dot(chosen, gv[g, c, q, 1], preferred_element_type=F32)
                av[g, :, q] = total.reshape(REQ, 8, 256)

        landed(g)
        if turn > 0:
            deliver(turn - 1)
        with jax.named_scope(f"product{g}"):
            fence()
            product = jnp.zeros((COLS, 256), F32)
            seen_left = jnp.int32(0)
            seen_right = jnp.int32(0)
            for half in range(2):
                blocks = []
                for j in range(half * 8, half * 8 + 8):
                    source = wanted[g * REQ + j, me]
                    owner = source >> 4
                    on_left = owner == lat * N_LON + left
                    on_me = owner == me
                    from_left = halos[g][0, seen_left & 7]
                    from_right = halos[g][1, seen_right & 7]
                    from_me = fld[g * STILES + (source & 15)]
                    blocks.append(
                        jnp.where(on_me, from_me, jnp.where(on_left, from_left, from_right))
                    )
                    seen_left = seen_left + jnp.where(on_left, 1, 0)
                    seen_right = seen_right + jnp.where(on_left | on_me, 0, 1)
                turned = jnp.concatenate(blocks, axis=0).T
                source = av[g, pl.ds(half * 8, 8)].reshape(256, 256)
                high = source.astype(BF16)
                low = (source - high.astype(F32)).astype(BF16)
                product += jnp.dot(turned, high, preferred_element_type=F32)
                product += jnp.dot(turned, low, preferred_element_type=F32)
            by_model = product.reshape(COLS // MONTHS, MONTHS, 256)
            centred = by_model - jnp.sum(by_model, axis=1, keepdims=True) * (1.0 / MONTHS)
            centred = centred.reshape(COLS, 256)
            pv[0, pl.ds(g * COLS, COLS), :] = centred[:, :128]
            pv[1, pl.ds(g * COLS, COLS), :] = centred[:, 128:]

        with jax.named_scope(f"pack{g}"):

            @pl.loop(start, stop, unroll=True)
            def _(i):
                base = pl.multiple_of(i * 72, 8)
                last = [pv[half, pl.ds(base + 8, 8, stride=9), :] for half in range(2)]
                for r, (half, shift) in enumerate(((0, 72), (0, 16), (0, 88), (1, 72), (1, 16))):
                    tails[i, pl.ds(r, 8, stride=8), :] = pltpu.roll(last[half], shift, 1)
                for r in range(5, 8):
                    tails[i, pl.ds(r, 8, stride=8), :] = jnp.zeros((8, 128), F32)
                for j in range(8):
                    first = pv[0, pl.ds(base + 9 * j, 8), :]
                    second = jnp.where(
                        lanes < 72, pv[1, pl.ds(base + 9 * j, 8), :], tails[i, 8 * j : 8 * j + 8, :]
                    )
                    pairbox[j & 1, i * 4 + j // 2] = jnp.concatenate([first, second], axis=0)

            pair_copy(turn).start()

    deliver(GRIDS - 1)

    with jax.named_scope("arrive"):
        inbox[chip] = outbox[chip]
        everything = pltpu.make_async_remote_copy(
            src_ref=outbox,
            dst_ref=inbox.at[pl.ds(0, CHIPS)],
            send_sem=rs_s,
            recv_sem=rs_r,
            device_id=(lat, right),
            device_id_type=MESH,
        )
        everything.wait_recv()
    with jax.named_scope("final"):
        total = jnp.zeros((16, 128), F32)
        for i in range(CHIPS):
            total += inbox[i].astype(F32)
        first, second = total[:8], total[8:]
        by_56, by_112, by_40 = (pltpu.roll(second, shift, 1) for shift in (56, 112, 40))
        lane = lanes[:1]
        last_0 = jnp.where(lane < 56, by_56[0:1], jnp.where(lane < 112, by_112[1:2], by_40[2:3]))
        last_1 = jnp.where(lane < 56, by_56[3:4], by_112[4:5])
        out[0:8, 0:128] = first
        out[0:8, 128:EOFS] = second[:, : EOFS - 128]
        out[8:9, 0:128] = last_0
        out[8:9, 128:EOFS] = last_1[:, : EOFS - 128]

    with jax.named_scope("drain"):
        everything.wait_send()
        for g in range(GRIDS):
            halo_copy(0, g).wait_send()
            halo_copy(1, g).wait_send()
            pair_copy(g).wait_send()


def shards(fields, weights, pair_slots, pair_counts, requests, eofs):
    return pl.pallas_call(
        body,
        out_shape=pltpu.VMEM((OWN, EOFS), F32),
        in_specs=[pl.BlockSpec(memory_space=pl.ANY)] * 6,
        out_specs=pl.BlockSpec(memory_space=pltpu.VMEM),
        scratch_shapes=[
            pltpu.SMEM((GRIDS * REQ, DEVS), jnp.int32),
            pltpu.VMEM((GRIDS, PAIRS, TILES), jnp.int32),
            pltpu.VMEM((GRIDS, TILES), jnp.int32),
            pltpu.VMEM((GRIDS * STILES, TS, COLS), BF16),
            pltpu.VMEM((2, GRIDS, CAP, TS, COLS), BF16),
            pltpu.VMEM((2, CAP, TS, COLS), BF16),
            pltpu.VMEM((2, CAP, TS, COLS), BF16),
            pltpu.VMEM((2, CAP, TS, COLS), BF16),
            pltpu.VMEM((GROUPS, 4, GRIDS, 256, TT), BF16),
            pltpu.VMEM((GROUPS, 256, 512), BF16),
            pltpu.VMEM((GRIDS, GROUPS, 4, 2, 256, 256), BF16),
            pltpu.VMEM((GRIDS * GROUPS, 128, 256), BF16),
            pltpu.VMEM((GRIDS, REQ, 4, 8, 256), F32),
            pltpu.VMEM((2, GRIDS * COLS + 8, 128), F32),
            pltpu.VMEM((16, 64, 128), F32),
            pltpu.VMEM((2, CHIPS, 16, 128), F32),
            pltpu.VMEM((CHIPS, 16, 128), F32),
            pltpu.VMEM((CHIPS, 16, 128), BF16),
            pltpu.VMEM((CHIPS + 1, 16, 128), BF16),
            pltpu.SemaphoreType.DMA((3,)),
            pltpu.SemaphoreType.DMA,
            pltpu.SemaphoreType.DMA((GROUPS, 4)),
            pltpu.SemaphoreType.DMA((GROUPS,)),
            pltpu.SemaphoreType.DMA((2, GRIDS)),
            pltpu.SemaphoreType.DMA((2, GRIDS)),
            pltpu.SemaphoreType.REGULAR,
            pltpu.SemaphoreType.REGULAR,
            pltpu.SemaphoreType.REGULAR,
            pltpu.SemaphoreType.REGULAR,
            pltpu.SemaphoreType.DMA((GRIDS,)),
            pltpu.SemaphoreType.DMA((GRIDS,)),
            pltpu.SemaphoreType.DMA,
            pltpu.SemaphoreType.DMA,
        ],
        compiler_params=pltpu.CompilerParams(
            collective_id=0, has_side_effects=True, vmem_limit_bytes=56 * 1024 * 1024
        ),
    )(
        requests.transpose(0, 2, 1).reshape(GRIDS * REQ, DEVS),
        pair_slots.transpose(0, 2, 1),
        pair_counts,
        fields.reshape(GRIDS * STILES, TS, COLS),
        weights.reshape(GRIDS, TILES, PAIRS * TS, TT),
        eofs,
    ).T


def solution(mesh):
    return jax.shard_map(
        shards,
        mesh=mesh,
        in_specs=(
            P(None, ("lat", "lon"), None, None),
            P(None, ("lat", "lon"), None, None, None),
            P(None, ("lat", "lon"), None),
            P(None, ("lat", "lon")),
            P(),
            P(None, ("lat", "lon")),
        ),
        out_specs=P(None, ("lat", "lon")),
        check_vma=False,
    )
```
